32 devices in a mesh: dp: 8 (over z, x), shard: 4 (over y, core).
Axes of the slice: x: 2, y: 2, z: 4, core: 2. Of those that a mesh axis runs over, the one named last changes fastest.
Arguments:
- tokens: bfloat16 [128, 3584], P('dp', 'shard'), may hold values from -6 to 6
- targets: bfloat16 [128, 3584], P('dp', 'shard'), may hold values from -6 to 6
- task_of_token: int32 [128], P('dp'), may hold values from 0 to 15, never falling along the last dimension, each value on 1 to 16 neighbouring positions
- up_weight: bfloat16 [18944, 3584], P('dp', 'shard'), may hold values from -0.09375 to 0.09375
- down_weight: bfloat16 [18944, 3584], P('dp', 'shard'), may hold values from -0.046875 to 0.046875
- outer_up: bfloat16 [18944, 3584], P('dp', 'shard'), may hold values from -6 to 6
- outer_down: bfloat16 [18944, 3584], P('dp', 'shard'), may hold values from -6 to 6
Outputs:
- meta_up: float32 [18944, 3584], P('dp', 'shard')
- meta_down: float32 [18944, 3584], P('dp', 'shard')
The draws below stay inside these ranges and needn't reach their ends.
Inputs may be any that keep to these rules, and one draw needn't show every extreme that they name: `task_of_token`: task numbers never fall along the tokens; every task has 1 to 16 tokens, and some task has exactly 16.
All inputs are finite; a program needn't handle non-finite values.
Results may differ from the reference program's by a relative error of at most 0.001.
Values may be sent and summed in bfloat16 or wider, within the bound.
A program may use at most 64 MiB of HBM per device.

```python
import math
import jax
import jax.numpy as jnp
import numpy as np
from jax import lax

D = 3584
FF = 18944
TASKS = 16
ITERS = 2
TOKENS = 128
MOST = 16


def level_of(own_key, extent, shards, smallest, high):
    gain = 1.0
    for position, parts in shards:
        draws = jax.random.uniform(jax.random.fold_in(jax.random.fold_in(own_key, 6), position), (parts,), jnp.float32, smallest / len(shards), high / len(shards))
        gain = gain * jnp.repeat(jnp.exp(draws), extent[position] // parts).reshape((-1,) + (1,) * (len(extent) - 1 - position))
    return gain


def profile(number_of, total, reach, skew):
    portions = [(1 << 20) // math.isqrt(rank ** skew) + 1 for rank in range(2, number_of + 1)]
    spare, holding = total - reach - (number_of - 1), [1] * (number_of - 1)
    while spare > 0:
        candidates = [i for i in range(number_of - 1) if holding[i] < reach]
        whole, left = sum([portions[i] for i in candidates]), spare
        for i in candidates:
            extra = min(reach - holding[i], max(1, left * portions[i] // whole), spare)
            holding[i] = holding[i] + extra
            spare = spare - extra
    return np.array([reach] + holding)


def ragged(key, count, total, most, skew):
    if count == 2:
        one = jax.random.randint(key, (), max(1, total - most), min(most, total - 1) + 1)
        return jnp.stack([one, total - one])
    lengths = jnp.asarray(profile(count, total, most, skew), jnp.int32)
    twos = (count - 1) // 2
    giver, sink = lengths[1:1 + 2 * twos:2], lengths[2:2 + 2 * twos:2]
    margin = jnp.minimum(giver - 1, most - sink)
    shifted = jax.random.randint(jax.random.fold_in(key, 1), (twos,), 0, 1 << 20) % (margin + 1)
    lengths = lengths.at[1:1 + 2 * twos:2].set(giver - shifted).at[2:2 + 2 * twos:2].set(sink + shifted)
    return lengths[jax.random.permutation(jax.random.fold_in(key, 2), count)]


def gaussian(rng, shape, scale, most, shards=(), held_as=jnp.bfloat16):
    array = scale * jax.random.normal(rng, shape, jnp.float32)
    if shards:
        array = array * level_of(rng, shape, shards, -0.22, 0.18)
    return jnp.clip(array, -most, most).astype(held_as)


def setup_inputs(seed: int = 0) -> dict:
    splits = jax.random.split(jax.random.key(seed), 8)
    return {
        "tokens": gaussian(splits[0], (TOKENS, D), 1.0, 6.0, ((0, 8), (1, 4))),
        "targets": gaussian(splits[1], (TOKENS, D), 1.0, 6.0, ((0, 8), (1, 4))),
        "task_of_token": jnp.searchsorted(jnp.cumsum(ragged(splits[2], TASKS, TOKENS, MOST, 0)), jnp.arange(TOKENS), side="right").astype(jnp.int32),
        "up_weight": gaussian(splits[3], (FF, D), D ** -0.5, 0.09375, ((0, 8), (1, 4))),
        "down_weight": gaussian(splits[4], (FF, D), FF ** -0.5, 0.046875, ((0, 8), (1, 4))),
        "outer_up": gaussian(splits[5], (FF, D), 1.0, 6.0, ((0, 8), (1, 4))),
        "outer_down": gaussian(splits[6], (FF, D), 1.0, 6.0, ((0, 8), (1, 4))),
    }


def sigmoid_parts(linear_part):
    argument = linear_part.astype(jnp.float32)
    logistic = jax.nn.sigmoid(argument)
    derivative = logistic * (1.0 + argument * (1.0 - logistic))
    second_order = logistic * (1.0 - logistic) * (2.0 + argument * (1.0 - 2.0 * logistic))
    return argument * logistic, derivative, second_order


def contract_last(left_side, right_side):
    return lax.dot_general(left_side, right_side, (((1,), (1,)), ((), ())), preferred_element_type=jnp.float32)


def contract_first(left_side, right_side):
    return lax.dot_general(left_side, right_side, (((0,), (0,)), ((), ())), preferred_element_type=jnp.float32)


def stored(values):
    return lax.optimization_barrier(values.astype(jnp.bfloat16))


def reference(tokens, targets, task_of_token, up_weight, down_weight, outer_up, outer_down):
    task_index = jnp.arange(TASKS, dtype=jnp.int32)
    members = (task_of_token[:, None] == task_index[None, :]).astype(jnp.float32)
    task_counts = jnp.sum(members, axis=0)
    inverse = 1.0 / (TASKS * task_counts)
    weight = jnp.sum(members * inverse[None, :], axis=1)
    linear_part = stored(contract_last(tokens, up_weight))
    activation, derivative, second_order = sigmoid_parts(linear_part)
    hidden = activation.astype(jnp.bfloat16)
    output_rows = jnp.dot(hidden, down_weight, preferred_element_type=jnp.float32)
    errors = (weight[:, None] * (output_rows - targets.astype(jnp.float32))).astype(jnp.bfloat16)
    backward = stored(contract_last(errors, down_weight)).astype(jnp.float32)

    def operator(vector_up, vector_down):
        direction_up = vector_up.astype(jnp.bfloat16)
        direction_down = vector_down.astype(jnp.bfloat16)
        tangent_linear = stored(contract_last(tokens, direction_up)).astype(jnp.float32)
        tangent_hidden = (derivative * tangent_linear).astype(jnp.bfloat16)
        tangent_output = jnp.dot(tangent_hidden, down_weight, preferred_element_type=jnp.float32)
        tangent_output = tangent_output + jnp.dot(hidden, direction_down, preferred_element_type=jnp.float32)
        tangent_errors = (weight[:, None] * tangent_output).astype(jnp.bfloat16)
        tangent_backward = stored(contract_last(tangent_errors, down_weight) + contract_last(errors, direction_down))
        tangent_gate = (derivative * tangent_backward.astype(jnp.float32) + second_order * backward * tangent_linear).astype(jnp.bfloat16)
        hessian_up = contract_first(tangent_gate, tokens)
        hessian_down = contract_first(tangent_hidden, errors) + contract_first(hidden, tangent_errors)
        return vector_up + hessian_up, vector_down + hessian_down

    residual_up = outer_up.astype(jnp.float32)
    residual_down = outer_down.astype(jnp.float32)
    solution_up = jnp.zeros_like(residual_up)
    solution_down = jnp.zeros_like(residual_down)
    search_up, search_down = residual_up, residual_down
    norm_now = jnp.sum(residual_up * residual_up) + jnp.sum(residual_down * residual_down)
    for iteration in range(ITERS):
        image_up, image_down = operator(search_up, search_down)
        step_size = norm_now / (jnp.sum(search_up * image_up) + jnp.sum(search_down * image_down))
        solution_up = solution_up + step_size * search_up
        solution_down = solution_down + step_size * search_down
        residual_up = residual_up - step_size * image_up
        residual_down = residual_down - step_size * image_down
        norm_next = jnp.sum(residual_up * residual_up) + jnp.sum(residual_down * residual_down)
        ratio_next = norm_next / norm_now
        search_up = residual_up + ratio_next * search_up
        search_down = residual_down + ratio_next * search_down
        norm_now = norm_next
    return solution_up, solution_down
```

```python
import functools

import jax
import jax.numpy as jnp
from jax import lax
from jax.experimental import pallas as pl
from jax.experimental.pallas import tpu as pltpu
from jax.sharding import PartitionSpec as P

TASKS = 16
BF = jnp.bfloat16
F32 = jnp.float32
MESH = pl.DeviceIdType.MESH
VM = pl.BlockSpec(memory_space=pltpu.VMEM)


def sigmoid_parts(linear_part):
    argument = linear_part.astype(F32)
    logistic = jax.nn.sigmoid(argument)
    derivative = logistic * (1.0 + argument * (1.0 - logistic))
    second_order = logistic * (1.0 - logistic) * (2.0 + argument * (1.0 - 2.0 * logistic))
    return (argument * logistic, derivative, second_order)


def contract_last(left_side, right_side):
    return lax.dot_general(
        left_side, right_side, (((1,), (1,)), ((), ())), preferred_element_type=F32
    )


def contract_first(left_side, right_side):
    return lax.dot_general(
        left_side, right_side, (((0,), (0,)), ((), ())), preferred_element_type=F32
    )


def product(left_side, right_side):
    return jnp.dot(left_side, right_side, preferred_element_type=F32)


def remote(src, dst, send_sem, recv_sem, where):
    return pltpu.make_async_remote_copy(
        src_ref=src,
        dst_ref=dst,
        send_sem=send_sem,
        recv_sem=recv_sem,
        device_id=where,
        device_id_type=MESH,
    )


def greet(places):
    barrier = pltpu.get_barrier_semaphore()
    for place in places:
        pl.semaphore_signal(barrier, inc=1, device_id=place, device_id_type=MESH)
    pl.semaphore_wait(barrier, len(places))


def rows_at(index, count):
    return pl.ds(pl.multiple_of(index * count, count), count)


def call(kernel, outs, scratch, number, args):
    return pl.pallas_call(
        kernel,
        out_shape=outs,
        in_specs=[VM] * len(args),
        out_specs=[VM] * len(outs),
        scratch_shapes=scratch,
        compiler_params=pltpu.CompilerParams(
            collective_id=number, has_side_effects=True, vmem_limit_bytes=48 * 2**20
        ),
    )(*args)


def ring_places(axis, n):
    me = lax.axis_index(axis)
    return me, [{axis: lax.rem(me + k, n)} for k in range(1, n)], [
        lax.rem(me + k, n) for k in range(1, n)
    ]


def gather_kernel(n, count, *refs):
    ins, outs = refs[:count], refs[count : 2 * count]
    send_sem, recv_sem = refs[2 * count :]
    me, places, _ = ring_places("dp", n)
    for src, dst in zip(ins, outs):
        dst[rows_at(me, src.shape[0]), :] = src[...]
    greet(places)
    copies = []
    for k, place in enumerate(places):
        for i, (src, dst) in enumerate(zip(ins, outs)):
            rows = rows_at(me, src.shape[0])
            copies.append(
                remote(src, dst.at[rows, :], send_sem.at[i, k], recv_sem.at[i, k], place)
            )
            copies[-1].start()
    for copy in copies:
        copy.wait()


def gather_dp(n, number, *arrays):
    count = len(arrays)
    outs = [jax.ShapeDtypeStruct((n * a.shape[0], a.shape[1]), a.dtype) for a in arrays]
    sems = [pltpu.SemaphoreType.DMA((count, n - 1))] * 2
    return call(functools.partial(gather_kernel, n, count), outs, sems, number, arrays)


def sum_kernel(n, count, bits, *refs):
    ins, outs = refs[:count], refs[count : 2 * count]
    halves, accs, wires = (refs[(2 + j) * count : (3 + j) * count] for j in range(3))
    send_sem, recv_sem = refs[5 * count :]
    me = lax.axis_index("shard")

    def flip(bit):
        step = 1 << bit
        return {"shard": me + step - 2 * step * lax.rem(me // step, 2)}

    greet([flip(bit) for bit in range(bits)])
    low = lax.rem(me, 2)
    first = []
    for i in range(count):
        half = ins[i].shape[0] // 2
        first.append(
            remote(
                ins[i].at[rows_at(1 - low, half), :],
                halves[i],
                send_sem.at[i, 0],
                recv_sem.at[i, 0],
                flip(0),
            )
        )
        first[-1].start()
    now = []
    for i in range(count):
        half = ins[i].shape[0] // 2
        first[i].wait()
        total = ins[i][rows_at(low, half), :].astype(F32) + halves[i][...].astype(F32)
        accs[i][0] = total.astype(ins[i].dtype)
        if bits > 1:
            copy = remote(
                accs[i].at[0], wires[i].at[0], send_sem.at[i, 1], recv_sem.at[i, 1], flip(1)
            )
            copy.start()
            now.append(copy)
    last = []
    for i in range(count):
        half = ins[i].shape[0] // 2
        mine = rows_at(low, half)
        for bit in range(1, bits):
            now[i].wait()
            total = accs[i][bit - 1].astype(F32) + wires[i][bit - 1].astype(F32)
            accs[i][bit] = total.astype(ins[i].dtype)
            if bit + 1 < bits:
                now[i] = remote(
                    accs[i].at[bit],
                    wires[i].at[bit],
                    send_sem.at[i, bit + 1],
                    recv_sem.at[i, bit + 1],
                    flip(bit + 1),
                )
                now[i].start()
        outs[i][mine, :] = accs[i][bits - 1]
        copy = remote(
            accs[i].at[bits - 1],
            outs[i].at[mine, :],
            send_sem.at[i, bits],
            recv_sem.at[i, bits],
            flip(0),
        )
        copy.start()
        last.append(copy)
    for copy in last:
        copy.wait()


def sum_shard(n, number, *arrays):
    count = len(arrays)
    bits = n.bit_length() - 1
    outs = [jax.ShapeDtypeStruct(a.shape, a.dtype) for a in arrays]
    sizes = [(a.shape[0] // 2, a.shape[1]) for a in arrays]
    scratch = [pltpu.VMEM(s, a.dtype) for s, a in zip(sizes, arrays)]
    scratch += [pltpu.VMEM((bits,) + s, a.dtype) for s, a in zip(sizes, arrays)]
    scratch += [pltpu.VMEM((max(bits - 1, 1),) + s, a.dtype) for s, a in zip(sizes, arrays)]
    scratch += [pltpu.SemaphoreType.DMA((count, bits + 1))] * 2
    return call(functools.partial(sum_kernel, n, count, bits), outs, scratch, number, arrays)


def error_kernel(
    n, y_ref, z_ref, targets_ref, weight_ref, e_ref, t_ref, row_ref,
    held, fresh, send_sem, recv_sem, send_two, recv_two,
):
    rows = targets_ref.shape[0]
    me, places, peers = ring_places("dp", n)
    greet(places)
    copies = []
    for i, part in enumerate((y_ref, z_ref)):
        for k in range(n - 1):
            copy = remote(
                part.at[rows_at(peers[k], rows), :],
                held.at[i, k],
                send_sem.at[i, k],
                recv_sem.at[i, k],
                places[k],
            )
            copy.start()
            copies.append(copy)
    mine = rows_at(me, rows)
    weight = weight_ref[:, 0:1]
    second = []
    for i, part in enumerate((y_ref, z_ref)):
        total = part[mine, :].astype(F32)
        for k in range(n - 1):
            copies[i * (n - 1) + k].wait()
            total = total + held[i, k].astype(F32)
        if i == 0:
            value = (weight * (total - targets_ref[...].astype(F32))).astype(BF)
        else:
            row_ref[...] = total
            value = (weight * total).astype(BF)
        dst = (e_ref, t_ref)[i]
        fresh[i] = value
        dst[mine, :] = value
        for k in range(n - 1):
            copy = remote(
                fresh.at[i], dst.at[mine, :], send_two.at[i, k], recv_two.at[i, k], places[k]
            )
            copy.start()
            second.append(copy)
    for copy in second:
        copy.wait()


def all_errors(n, number, y, z, targets, weight):
    rows, width = targets.shape
    outs = [jax.ShapeDtypeStruct(y.shape, BF)] * 2 + [jax.ShapeDtypeStruct((rows, width), F32)]
    scratch = [pltpu.VMEM((2, n - 1, rows, width), BF), pltpu.VMEM((2, rows, width), BF)]
    scratch += [pltpu.SemaphoreType.DMA((2, n - 1))] * 4
    return call(
        functools.partial(error_kernel, n), outs, scratch, number, (y, z, targets, weight)
    )


def totals_kernel(
    n, m, w_ref, row_ref, weight_ref, part_ref, out_ref,
    held, dp_slots, shard_slots, own, send_sem, recv_sem, send_two, recv_two, send_three, recv_three,
):
    rows = row_ref.shape[0]
    me, places, peers = ring_places("dp", n)
    own_shard, shard_places, _ = ring_places("shard", m)
    greet(places + shard_places)
    copies = []
    for k in range(n - 1):
        copy = remote(
            w_ref.at[rows_at(peers[k], rows), :],
            held.at[k],
            send_sem.at[k],
            recv_sem.at[k],
            places[k],
        )
        copy.start()
        copies.append(copy)
    total = w_ref[rows_at(me, rows), :].astype(F32)
    for k in range(n - 1):
        copies[k].wait()
        total = total + held[k].astype(F32)
    row, weight = row_ref[...], weight_ref[:, 0:1]
    index = lax.broadcasted_iota(jnp.int32, part_ref.shape, 0)
    value = part_ref[...]
    for place, term in ((1, row * row), (3, row * total), (4, total * total)):
        number = jnp.sum(jnp.sum(weight * term, axis=1, keepdims=True), axis=0, keepdims=True)
        value = value + jnp.where(index == place, number, 0.0)
    own[0] = value
    dp_slots[pl.ds(me, 1)] = value[None]
    copies = []
    for k in range(n - 1):
        copy = remote(
            own.at[0], dp_slots.at[me], send_two.at[k], recv_two.at[k], places[k]
        )
        copy.start()
        copies.append(copy)
    for copy in copies:
        copy.wait()
    value = dp_slots[0]
    for k in range(1, n):
        value = value + dp_slots[k]
    own[1] = value
    shard_slots[pl.ds(own_shard, 1)] = value[None]
    copies = []
    for k in range(m - 1):
        copy = remote(
            own.at[1],
            shard_slots.at[own_shard],
            send_three.at[k],
            recv_three.at[k],
            shard_places[k],
        )
        copy.start()
        copies.append(copy)
    for copy in copies:
        copy.wait()
    value = shard_slots[0]
    for k in range(1, m):
        value = value + shard_slots[k]
    out_ref[...] = value


def all_totals(n, m, number, w, row, weight, part):
    scratch = [
        pltpu.VMEM((n - 1,) + row.shape, BF),
        pltpu.VMEM((n,) + part.shape, F32),
        pltpu.VMEM((m,) + part.shape, F32),
        pltpu.VMEM((2,) + part.shape, F32),
    ]
    scratch += [pltpu.SemaphoreType.DMA((n - 1,))] * 4 + [pltpu.SemaphoreType.DMA((m - 1,))] * 2
    outs = [jax.ShapeDtypeStruct(part.shape, F32)]
    return call(
        functools.partial(totals_kernel, n, m), outs, scratch, number, (w, row, weight, part)
    )[0]


def two_halves(matrix):
    high = matrix.astype(BF)
    return high, (matrix - high.astype(F32)).astype(BF)


def body(n, m, tokens, targets, task_of_token, up_weight, down_weight, outer_up, outer_down):
    rows = tokens.shape[0]
    count = rows * n
    task_block = jnp.broadcast_to(task_of_token.astype(F32)[:, None], (rows, 128))
    gathered, all_tasks = gather_dp(n, 0, tokens, task_block)
    same = (task_block[:, 0:1] == all_tasks[:, 0][None, :]).astype(F32)
    weight = 1.0 / (TASKS * jnp.sum(same, axis=1, keepdims=True))
    weight = jnp.broadcast_to(weight, (rows, 128))

    linear_part, tangent_linear = sum_shard(
        m,
        1,
        contract_last(gathered, up_weight).astype(BF),
        contract_last(gathered, outer_up).astype(BF),
    )
    activation, derivative, second_order = sigmoid_parts(linear_part)
    hidden = activation.astype(BF)
    tangent = tangent_linear.astype(F32)
    tangent_hidden = (derivative * tangent).astype(BF)

    both = product(jnp.concatenate([hidden, tangent_hidden], axis=0), down_weight)
    errors, tangent_errors, tangent_row = all_errors(
        n,
        2,
        both[:count].astype(BF),
        (both[count:] + product(hidden, outer_down)).astype(BF),
        targets,
        weight,
    )

    two_errors = jnp.concatenate([errors, tangent_errors], axis=0)
    back = contract_last(two_errors, down_weight)
    backward = back[:count]
    through_outer = contract_last(errors, outer_down)
    curved = second_order * backward
    gate_part = derivative * (back[count:] + through_outer) + curved * tangent
    token_gram = contract_last(gathered, gathered)
    tangent_gate, full_gram = sum_shard(m, 3, gate_part.astype(BF), token_gram)

    high, low = two_halves(full_gram)
    lowered = product(
        jnp.concatenate([high, low], axis=1),
        jnp.concatenate([tangent_gate, tangent_gate], axis=0),
    )
    carried = (derivative * lowered).astype(BF)
    hidden_gram = contract_last(
        jnp.concatenate([hidden, carried], axis=0),
        jnp.concatenate([tangent_hidden, hidden], axis=0),
    )
    tangent_gram = contract_last(tangent_hidden, tangent_hidden)
    hidden_tangent, hidden_hidden = hidden_gram[:count, :count], hidden_gram[:count, count:]
    carried_tangent, carried_hidden = hidden_gram[count:, :count], hidden_gram[count:, count:]
    error_gram = contract_last(two_errors, two_errors)
    error_error, error_tangent = error_gram[:count, :count], error_gram[:count, count:]
    further = product(carried, down_weight) + product(
        jnp.concatenate([hidden_tangent, hidden_hidden], axis=1).astype(BF), two_errors
    )

    start_norm = jnp.sum(jnp.square(outer_up.astype(F32))) + jnp.sum(
        jnp.square(outer_down.astype(F32))
    )
    crossing = through_outer
    first_term = jnp.sum(
        2.0 * tangent_hidden.astype(F32) * crossing + curved * tangent * tangent
    )
    mixed_term = jnp.sum(carried.astype(F32) * crossing + curved * tangent * lowered)
    last_term = jnp.sum(curved * lowered * lowered)
    gate_gram = contract_last(tangent_gate, tangent_gate)
    s_e = jnp.sum(tangent_gram * error_error)
    h_t = jnp.sum(hidden_tangent.T * error_tangent)
    change_norm = (
        jnp.sum(gate_gram * token_gram)
        + s_e
        + 2.0 * h_t
        + jnp.sum(hidden_hidden * error_gram[count:, count:])
    )
    mixed_term = mixed_term + s_e + h_t
    last_term = last_term + 2.0 * (
        jnp.sum(carried_tangent * error_error) + jnp.sum(carried_hidden * error_tangent)
    )
    index = lax.broadcasted_iota(jnp.int32, (8, 128), 0)
    part = jnp.zeros((8, 128), F32)
    for place, value in enumerate((start_norm, first_term, change_norm, mixed_term, last_term)):
        part = part + jnp.where(index == place, value, 0.0)

    sums = all_totals(n, m, 4, further.astype(BF), tangent_row, weight, part)
    norm, first, change, mixed, final = (sums[i, 0] for i in range(5))
    step = norm / (norm + first)
    keep = first / (norm + first)
    norm_next = keep * keep * norm - 2.0 * keep * step * first + step * step * change
    ratio = norm_next / norm
    curvature = (
        norm_next
        + keep * keep * first
        - 2.0 * keep * step * mixed
        + step * step * final
        - ratio * norm_next / step
    )
    step_next = norm_next / curvature
    of_outer = step + step_next * (ratio + keep)
    of_change = -step_next * step
    change_up = contract_first(tangent_gate, gathered)
    change_down = contract_first(
        jnp.concatenate([tangent_hidden, hidden], axis=0), two_errors
    )
    return (
        of_outer * outer_up.astype(F32) + of_change * change_up,
        of_outer * outer_down.astype(F32) + of_change * change_down,
    )


def solution(mesh):
    placed = tuple(P("dp") if i == 2 else P("dp", "shard") for i in range(7))
    return jax.shard_map(
        functools.partial(body, mesh.shape["dp"], mesh.shape["shard"]),
        mesh=mesh,
        in_specs=placed,
        out_specs=(P("dp", "shard"), P("dp", "shard")),
        check_vma=False,
    )
```

```python
import functools

import jax
import jax.numpy as jnp
from jax import lax
from jax.experimental import pallas as pl
from jax.experimental.pallas import tpu as pltpu
from jax.sharding import PartitionSpec as P

TASKS = 16
BF = jnp.bfloat16
F32 = jnp.float32
MESH = pl.DeviceIdType.MESH
VM = pl.BlockSpec(memory_space=pltpu.VMEM)


def sigmoid_parts(linear_part):
    argument = linear_part.astype(F32)
    logistic = jax.nn.sigmoid(argument)
    derivative = logistic * (1.0 + argument * (1.0 - logistic))
    second_order = logistic * (1.0 - logistic) * (2.0 + argument * (1.0 - 2.0 * logistic))
    return (argument * logistic, derivative, second_order)


def contract_last(left_side, right_side):
    return lax.dot_general(
        left_side, right_side, (((1,), (1,)), ((), ())), preferred_element_type=F32
    )


def contract_first(left_side, right_side):
    return lax.dot_general(
        left_side, right_side, (((0,), (0,)), ((), ())), preferred_element_type=F32
    )


def product(left_side, right_side):
    return jnp.dot(left_side, right_side, preferred_element_type=F32)


def remote(src, dst, send_sem, recv_sem, where):
    return pltpu.make_async_remote_copy(
        src_ref=src,
        dst_ref=dst,
        send_sem=send_sem,
        recv_sem=recv_sem,
        device_id=where,
        device_id_type=MESH,
    )


def greet(places):
    barrier = pltpu.get_barrier_semaphore()
    for place in places:
        pl.semaphore_signal(barrier, inc=1, device_id=place, device_id_type=MESH)
    pl.semaphore_wait(barrier, len(places))


def rows_at(index, count):
    return pl.ds(pl.multiple_of(index * count, count), count)


def call(kernel, outs, scratch, number, args, far=0):
    return pl.pallas_call(
        kernel,
        out_shape=outs,
        in_specs=[pl.BlockSpec(memory_space=pl.ANY)] * far + [VM] * (len(args) - far),
        out_specs=[VM] * len(outs),
        scratch_shapes=scratch,
        compiler_params=pltpu.CompilerParams(
            collective_id=number, has_side_effects=True, vmem_limit_bytes=48 * 2**20
        ),
    )(*args)


def ring_places(axis, n):
    me = lax.axis_index(axis)
    return me, [{axis: lax.rem(me + k, n)} for k in range(1, n)], [
        lax.rem(me + k, n) for k in range(1, n)
    ]


def gather_kernel(
    n, count, up_ref, down_ref, *refs
):
    ins, outs, norm_ref = refs[:count], refs[count : 2 * count], refs[2 * count]
    held, load_sem, send_sem, recv_sem = refs[2 * count + 1 :]
    loads = [
        pltpu.make_async_copy(src, held.at[i], load_sem.at[i])
        for i, src in enumerate((up_ref, down_ref))
    ]
    for load in loads:
        load.start()
    me, places, _ = ring_places("dp", n)
    for src, dst in zip(ins, outs):
        dst[rows_at(me, src.shape[0]), :] = src[...]
    greet(places)
    copies = []
    for k, place in enumerate(places):
        for i, (src, dst) in enumerate(zip(ins, outs)):
            rows = rows_at(me, src.shape[0])
            copies.append(
                remote(src, dst.at[rows, :], send_sem.at[i, k], recv_sem.at[i, k], place)
            )
            copies[-1].start()
    size, width = up_ref.shape
    total = jnp.zeros((16, width), F32)
    for i, load in enumerate(loads):
        load.wait()

        def add(step, value, i=i):
            block = held[i, rows_at(step, 16), :].astype(F32)
            return value + block * block

        total = lax.fori_loop(0, size // 16, add, total)
    number = jnp.sum(jnp.sum(total, axis=1, keepdims=True), axis=0, keepdims=True)
    norm_ref[...] = jnp.broadcast_to(number, norm_ref.shape)
    for copy in copies:
        copy.wait()


def gather_dp(n, number, up, down, *arrays):
    count = len(arrays)
    outs = [jax.ShapeDtypeStruct((n * a.shape[0], a.shape[1]), a.dtype) for a in arrays]
    outs.append(jax.ShapeDtypeStruct((8, 128), F32))
    scratch = [pltpu.VMEM((2,) + up.shape, up.dtype), pltpu.SemaphoreType.DMA((2,))]
    scratch += [pltpu.SemaphoreType.DMA((count, n - 1))] * 2
    return call(
        functools.partial(gather_kernel, n, count), outs, scratch, number, (up, down) + arrays, 2
    )


def sum_kernel(n, count, bits, *refs):
    ins, outs = refs[:count], refs[count : 2 * count]
    halves, accs, wires = (refs[(2 + j) * count : (3 + j) * count] for j in range(3))
    send_sem, recv_sem = refs[5 * count :]
    me = lax.axis_index("shard")

    def flip(bit):
        step = 1 << bit
        return {"shard": me + step - 2 * step * lax.rem(me // step, 2)}

    greet([flip(bit) for bit in range(bits)])
    low = lax.rem(me, 2)
    first = []
    for i in range(count):
        half = ins[i].shape[0] // 2
        first.append(
            remote(
                ins[i].at[rows_at(1 - low, half), :],
                halves[i],
                send_sem.at[i, 0],
                recv_sem.at[i, 0],
                flip(0),
            )
        )
        first[-1].start()
    now = []
    for i in range(count):
        half = ins[i].shape[0] // 2
        first[i].wait()
        total = ins[i][rows_at(low, half), :].astype(F32) + halves[i][...].astype(F32)
        accs[i][0] = total.astype(ins[i].dtype)
        if bits > 1:
            copy = remote(
                accs[i].at[0], wires[i].at[0], send_sem.at[i, 1], recv_sem.at[i, 1], flip(1)
            )
            copy.start()
            now.append(copy)
    last = []
    for i in range(count):
        half = ins[i].shape[0] // 2
        mine = rows_at(low, half)
        for bit in range(1, bits):
            now[i].wait()
            total = accs[i][bit - 1].astype(F32) + wires[i][bit - 1].astype(F32)
            accs[i][bit] = total.astype(ins[i].dtype)
            if bit + 1 < bits:
                now[i] = remote(
                    accs[i].at[bit],
                    wires[i].at[bit],
                    send_sem.at[i, bit + 1],
                    recv_sem.at[i, bit + 1],
                    flip(bit + 1),
                )
                now[i].start()
        outs[i][mine, :] = accs[i][bits - 1]
        copy = remote(
            accs[i].at[bits - 1],
            outs[i].at[mine, :],
            send_sem.at[i, bits],
            recv_sem.at[i, bits],
            flip(0),
        )
        copy.start()
        last.append(copy)
    for copy in last:
        copy.wait()


def sum_shard(n, number, *arrays):
    count = len(arrays)
    bits = n.bit_length() - 1
    outs = [jax.ShapeDtypeStruct(a.shape, a.dtype) for a in arrays]
    sizes = [(a.shape[0] // 2, a.shape[1]) for a in arrays]
    scratch = [pltpu.VMEM(s, a.dtype) for s, a in zip(sizes, arrays)]
    scratch += [pltpu.VMEM((bits,) + s, a.dtype) for s, a in zip(sizes, arrays)]
    scratch += [pltpu.VMEM((max(bits - 1, 1),) + s, a.dtype) for s, a in zip(sizes, arrays)]
    scratch += [pltpu.SemaphoreType.DMA((count, bits + 1))] * 2
    return call(functools.partial(sum_kernel, n, count, bits), outs, scratch, number, arrays)


def error_kernel(
    n, y_ref, z_ref, targets_ref, weight_ref, e_ref, t_ref, row_ref,
    held, fresh, send_sem, recv_sem, send_two, recv_two,
):
    rows = targets_ref.shape[0]
    me, places, peers = ring_places("dp", n)
    greet(places)
    copies = []
    for i, part in enumerate((y_ref, z_ref)):
        for k in range(n - 1):
            copy = remote(
                part.at[rows_at(peers[k], rows), :],
                held.at[i, k],
                send_sem.at[i, k],
                recv_sem.at[i, k],
                places[k],
            )
            copy.start()
            copies.append(copy)
    mine = rows_at(me, rows)
    weight = weight_ref[:, 0:1]
    second = []
    for i, part in enumerate((y_ref, z_ref)):
        total = part[mine, :].astype(F32)
        for k in range(n - 1):
            copies[i * (n - 1) + k].wait()
            total = total + held[i, k].astype(F32)
        if i == 0:
            value = (weight * (total - targets_ref[...].astype(F32))).astype(BF)
        else:
            row_ref[...] = total
            value = (weight * total).astype(BF)
        dst = (e_ref, t_ref)[i]
        fresh[i] = value
        dst[mine, :] = value
        for k in range(n - 1):
            copy = remote(
                fresh.at[i], dst.at[mine, :], send_two.at[i, k], recv_two.at[i, k], places[k]
            )
            copy.start()
            second.append(copy)
    for copy in second:
        copy.wait()


def all_errors(n, number, y, z, targets, weight):
    rows, width = targets.shape
    outs = [jax.ShapeDtypeStruct(y.shape, BF)] * 2 + [jax.ShapeDtypeStruct((rows, width), F32)]
    scratch = [pltpu.VMEM((2, n - 1, rows, width), BF), pltpu.VMEM((2, rows, width), BF)]
    scratch += [pltpu.SemaphoreType.DMA((2, n - 1))] * 4
    return call(
        functools.partial(error_kernel, n), outs, scratch, number, (y, z, targets, weight)
    )


def totals_kernel(
    n, m, w_ref, row_ref, weight_ref, part_ref, norm_ref, hidden_ref, tangent_ref, gate_ref,
    token_ref, error_ref, out_ref,
    held, dp_slots, shard_slots, own, send_sem, recv_sem, send_two, recv_two, send_three, recv_three,
):
    rows = row_ref.shape[0]
    me, places, peers = ring_places("dp", n)
    own_shard, shard_places, _ = ring_places("shard", m)
    greet(places + shard_places)
    copies = []
    for k in range(n - 1):
        copy = remote(
            w_ref.at[rows_at(peers[k], rows), :],
            held.at[k],
            send_sem.at[k],
            recv_sem.at[k],
            places[k],
        )
        copy.start()
        copies.append(copy)
    count = gate_ref.shape[0]

    def summed(term):
        return jnp.sum(jnp.sum(term, axis=1, keepdims=True), axis=0, keepdims=True)

    head, tail = pl.ds(0, count), pl.ds(count, count)
    errors, crossed = error_ref[head, head], error_ref[tail, head]
    tangents = tangent_ref[...]
    s_e = summed(tangents * errors)
    h_t = summed(hidden_ref[head, head] * crossed)
    change = summed(gate_ref[...] * token_ref[...]) + s_e + 2.0 * h_t
    change = change + summed(hidden_ref[head, tail] * error_ref[tail, tail])
    carry = summed(hidden_ref[tail, head] * errors)
    carry = carry + summed(hidden_ref[tail, tail] * error_ref[head, tail])
    total = w_ref[rows_at(me, rows), :].astype(F32)
    for k in range(n - 1):
        copies[k].wait()
        total = total + held[k].astype(F32)
    row, weight = row_ref[...], weight_ref[:, 0:1]
    index = lax.broadcasted_iota(jnp.int32, part_ref.shape, 0)
    value = part_ref[...]
    for place, number in ((2, change), (3, s_e + h_t), (4, 2.0 * carry)):
        value = value + jnp.where(index == place, number, 0.0)
    value = value + jnp.where(index == 0, norm_ref[...], 0.0)
    for place, term in ((1, row * row), (3, row * total), (4, total * total)):
        number = summed(weight * term)
        value = value + jnp.where(index == place, number, 0.0)
    own[0] = value
    dp_slots[pl.ds(me, 1)] = value[None]
    copies = []
    for k in range(n - 1):
        copy = remote(
            own.at[0], dp_slots.at[me], send_two.at[k], recv_two.at[k], places[k]
        )
        copy.start()
        copies.append(copy)
    for copy in copies:
        copy.wait()
    value = dp_slots[0]
    for k in range(1, n):
        value = value + dp_slots[k]
    own[1] = value
    shard_slots[pl.ds(own_shard, 1)] = value[None]
    copies = []
    for k in range(m - 1):
        copy = remote(
            own.at[1],
            shard_slots.at[own_shard],
            send_three.at[k],
            recv_three.at[k],
            shard_places[k],
        )
        copy.start()
        copies.append(copy)
    for copy in copies:
        copy.wait()
    value = shard_slots[0]
    for k in range(1, m):
        value = value + shard_slots[k]
    own[2] = value
    norm, first, change, mixed, final = (own[2, i : i + 1, :] for i in range(5))
    step = norm / (norm + first)
    keep = first / (norm + first)
    norm_next = keep * keep * norm - 2.0 * keep * step * first + step * step * change
    ratio = norm_next / norm
    curvature = (
        norm_next
        + keep * keep * first
        - 2.0 * keep * step * mixed
        + step * step * final
        - ratio * norm_next / step
    )
    step_next = norm_next / curvature
    out_ref[0:1, :] = step + step_next * (ratio + keep)
    out_ref[1:2, :] = -step_next * step


def all_totals(n, m, number, w, row, weight, part, *others):
    scratch = [
        pltpu.VMEM((n - 1,) + row.shape, BF),
        pltpu.VMEM((n,) + part.shape, F32),
        pltpu.VMEM((m,) + part.shape, F32),
        pltpu.VMEM((3,) + part.shape, F32),
    ]
    scratch += [pltpu.SemaphoreType.DMA((n - 1,))] * 4 + [pltpu.SemaphoreType.DMA((m - 1,))] * 2
    outs = [jax.ShapeDtypeStruct((2, 128), F32)]
    return call(
        functools.partial(totals_kernel, n, m), outs, scratch, number, (w, row, weight, part) + others
    )[0]


def two_halves(matrix):
    high = matrix.astype(BF)
    return high, (matrix - high.astype(F32)).astype(BF)


def body(n, m, tokens, targets, task_of_token, up_weight, down_weight, outer_up, outer_down):
    rows = tokens.shape[0]
    count = rows * n
    task_block = jnp.broadcast_to(task_of_token.astype(F32)[:, None], (rows, 128))
    gathered, all_tasks, start_norm = gather_dp(n, 0, outer_up, outer_down, tokens, task_block)
    same = (task_block[:, 0:1] == all_tasks[:, 0][None, :]).astype(F32)
    weight = 1.0 / (TASKS * jnp.sum(same, axis=1, keepdims=True))
    weight = jnp.broadcast_to(weight, (rows, 128))

    linear_part, tangent_linear = sum_shard(
        m,
        1,
        contract_last(gathered, up_weight).astype(BF),
        contract_last(gathered, outer_up).astype(BF),
    )
    activation, derivative, second_order = sigmoid_parts(linear_part)
    hidden = activation.astype(BF)
    tangent = tangent_linear.astype(F32)
    tangent_hidden = (derivative * tangent).astype(BF)

    both = product(jnp.concatenate([hidden, tangent_hidden], axis=0), down_weight)
    errors, tangent_errors, tangent_row = all_errors(
        n,
        2,
        both[:count].astype(BF),
        (both[count:] + product(hidden, outer_down)).astype(BF),
        targets,
        weight,
    )

    two_errors = jnp.concatenate([errors, tangent_errors], axis=0)
    back = contract_last(two_errors, down_weight)
    backward = back[:count]
    through_outer = contract_last(errors, outer_down)
    curved = second_order * backward
    gate_part = derivative * (back[count:] + through_outer) + curved * tangent
    token_gram = contract_last(gathered, gathered)
    tangent_gate, full_gram = sum_shard(m, 3, gate_part.astype(BF), token_gram)

    high, low = two_halves(full_gram)
    lowered = product(
        jnp.concatenate([high, low], axis=1),
        jnp.concatenate([tangent_gate, tangent_gate], axis=0),
    )
    carried = (derivative * lowered).astype(BF)
    hidden_gram = contract_last(
        jnp.concatenate([hidden, carried], axis=0),
        jnp.concatenate([tangent_hidden, hidden], axis=0),
    )
    tangent_gram = contract_last(tangent_hidden, tangent_hidden)
    error_gram = contract_last(two_errors, two_errors)
    further = product(carried, down_weight) + product(
        hidden_gram[:count].astype(BF), two_errors
    )

    crossing = through_outer
    first_term = jnp.sum(
        2.0 * tangent_hidden.astype(F32) * crossing + curved * tangent * tangent
    )
    mixed_term = jnp.sum(carried.astype(F32) * crossing + curved * tangent * lowered)
    last_term = jnp.sum(curved * lowered * lowered)
    gate_gram = contract_last(tangent_gate, tangent_gate)
    index = lax.broadcasted_iota(jnp.int32, (8, 128), 0)
    part = jnp.zeros((8, 128), F32)
    for place, value in ((1, first_term), (3, mixed_term), (4, last_term)):
        part = part + jnp.where(index == place, value, 0.0)

    sums = all_totals(
        n,
        m,
        4,
        further.astype(BF),
        tangent_row,
        weight,
        part,
        start_norm,
        hidden_gram,
        tangent_gram,
        gate_gram,
        token_gram,
        error_gram,
    )
    of_outer, of_change = sums[0, 0], sums[1, 0]
    change_up = contract_first(tangent_gate, gathered)
    change_down = contract_first(
        jnp.concatenate([tangent_hidden, hidden], axis=0), two_errors
    )
    return (
        of_outer * outer_up.astype(F32) + of_change * change_up,
        of_outer * outer_down.astype(F32) + of_change * change_down,
    )


def solution(mesh):
    placed = tuple(P("dp") if i == 2 else P("dp", "shard") for i in range(7))
    return jax.shard_map(
        functools.partial(body, mesh.shape["dp"], mesh.shape["shard"]),
        mesh=mesh,
        in_specs=placed,
        out_specs=(P("dp", "shard"), P("dp", "shard")),
        check_vma=False,
    )
```
